32 devices in a mesh: mat: 4 (over y, z), dp: 8 (over x, core).
Axes of the slice: x: 4, y: 2, z: 2, core: 2. Of those that a mesh axis runs over, the one named last changes fastest.
The devices are a block of a 4x4x8 slice.
Arguments:
- a_mat: bfloat16 [14336, 32768], P('mat', 'dp'), parts along dimension 0
Outputs:
- output: float32 [32, 5, 448, 448], P(('mat', 'dp')), parts along dimension 0
There are 4 independent parts. The reference program is written for one: setup_inputs(seed, part) draws one part's arguments, and reference() takes and returns one part's arrays. A program takes and returns all parts, laid end to end along the dimension named above; each array names one.
All inputs are finite; a program needn't handle non-finite values.
Results may differ from the reference program's by a relative error of at most 0.001.
Values are sent between devices in bfloat16 or wider.
A program may use at most 768 MiB of HBM per device.

```python
import jax
import jax.numpy as jnp
from jax import lax

GRAM_ORDER = 3584
COLS_DEV = 4096
GROUPS = 8
MIX_RANK = 8

BLOCK = GRAM_ORDER // GROUPS
SLOTS = GROUPS // 2 + 1
WIDTH = COLS_DEV * GROUPS


def pair_table():
    half = GROUPS // 2
    hi_list = []
    lo_list = []
    for dev_index in range(GROUPS):
        for slot in range(SLOTS):
            other_id = (dev_index - slot) % GROUPS
            if slot < half or dev_index < half:
                hi_list.append(max(dev_index, other_id))
                lo_list.append(min(dev_index, other_id))
            else:
                hi_list.append(-1)
                lo_list.append(-1)
    return jnp.array(hi_list, dtype=jnp.int32), jnp.array(lo_list, dtype=jnp.int32)


def setup_inputs(seed: int = 0, part: int = 0) -> dict:
    key = jax.random.fold_in(jax.random.key(seed), part)
    key_mix, key_src, key_gain = jax.random.split(key, 3)
    mixers = jax.random.normal(key_mix, (GROUPS, GRAM_ORDER, MIX_RANK), jnp.float32) * MIX_RANK ** -0.5
    sources = jax.random.normal(key_src, (GROUPS, MIX_RANK, COLS_DEV), jnp.float32)
    block_gain = jax.random.uniform(key_gain, (GROUPS,), jnp.float32, minval=0.7, maxval=1.4)
    row_gain = jnp.repeat(block_gain, BLOCK)
    mixed = jnp.einsum('snr,srk->nsk', mixers, sources).reshape(GRAM_ORDER, WIDTH)
    scale = (MIX_RANK ** 0.5 / (COLS_DEV * GROUPS ** 0.5)) ** 0.5
    a_mat = mixed * (row_gain[:, None] * scale)
    return {'a_mat': a_mat.astype(jnp.bfloat16)}


def reference(a_mat):
    hi_ids, lo_ids = pair_table()

    def one_block(pair_ids):
        hi_id, lo_id = pair_ids
        hi_rows = lax.dynamic_slice_in_dim(a_mat, jnp.maximum(hi_id, 0) * BLOCK, BLOCK, axis=0)
        lo_rows = lax.dynamic_slice_in_dim(a_mat, jnp.maximum(lo_id, 0) * BLOCK, BLOCK, axis=0)
        block_prod = jnp.dot(hi_rows, lo_rows.T, preferred_element_type=jnp.float32)
        return jnp.where(hi_id >= 0, block_prod, 0.0)

    blocks = lax.map(one_block, (hi_ids, lo_ids))
    return blocks.reshape(GROUPS, SLOTS, BLOCK, BLOCK)
```

```python
import functools

import jax
import jax.numpy as jnp
from jax import lax
from jax.experimental import pallas as pl
from jax.experimental.pallas import tpu as pltpu
from jax.sharding import PartitionSpec as P

CORES = 2
LANES = 128
O_SLOTS = 4
MESH = pl.DeviceIdType.MESH


def _kernel(groups, blk, a_hbm, out_hbm, a, x, ring, outgoing, acc, stage,
            load_sem, pair_send, pair_recv, ring_send, ring_recv, out_sem):
    chips = groups // CORES
    half_groups = groups // 2
    slots = half_groups + 1
    steps = chips - 1
    per_step = 2 * slots
    n_items = chips * per_step
    wide = 2 * LANES
    mid = blk // 2
    rows_l, rows_s = 2 * blk, blk + mid
    edge = blk - LANES
    low = blk - wide
    rows_dl, rows_ds = 2 * blk - LANES, LANES + low // 2
    blk_rows = rows_l + rows_s
    ring_rows = half_groups // 2 * blk_rows + rows_l
    tail = edge - wide

    me = lax.axis_index("dp")
    chip, core = me // CORES, me % CORES
    partner = chip * CORES + 1 - core
    chip_up = (chip + 1) % chips
    chip_down = (chip + chips - 1) % chips
    up, down = chip_up * CORES + core, chip_down * CORES + core

    def row_block(index):
        return pl.ds(pl.multiple_of(index * blk, 64), blk)

    def load(index):
        return pltpu.make_async_copy(a_hbm.at[row_block(index)], a.at[row_block(index)], load_sem.at[index])

    first = (chip_down * CORES + 1 - core, chip_up * CORES + 1 - core, chip_down * CORES + core, chip_up * CORES + core)
    chip_far = (chip + 2) % chips
    rest = (chip * CORES + 1 - core, chip * CORES + core, chip_far * CORES + 1 - core, chip_far * CORES + core)
    for index in first + rest:
        load(index).start()

    barrier = pltpu.get_barrier_semaphore()
    for other in (partner, up, down):
        pl.semaphore_signal(barrier, inc=1, device_id={"dp": other}, device_id_type=MESH)
    pl.semaphore_wait(barrier, 3)

    def item(n):
        step = n // per_step
        rest_n = n % per_step
        slot, way = rest_n // 2, rest_n % 2
        dest = (chip + 2 * chips + (1 + step) * (2 * way - 1)) % chips
        valid = jnp.logical_or(slot < half_groups, dest < chips // 2)
        return step, slot, way, dest, (slot + way) % 2, valid

    def by_case(slot, half, fn):
        for diag in (True, False):
            for part in (0, 1):
                cond = jnp.logical_and((slot == 0) if diag else (slot > 0), half == part)
                rows = ((rows_dl, rows_ds) if diag else (rows_l, rows_s))[part]
                pl.when(cond)(functools.partial(fn, diag, part, rows))

    def multiply(dest, parity, slot, half):
        p = dest * CORES + parity
        q = (p - slot + groups) % groups
        wrapped = (slot + groups - 1 - p) // groups
        hi = p + wrapped * (q - p)
        lo = q + wrapped * (p - q)
        left = a[row_block(hi), :]
        right = a[pl.ds(pl.multiple_of(lo * blk + half * (blk - wide), 64), wide), :]
        acc[...] = lax.dot_general(left, right, (((1,), (1,)), ((), ())), preferred_element_type=jnp.float32)

    def emit(diag, part, put):
        if part == 0:
            skip = LANES if diag else 0
            put(0, acc[:, :LANES])
            put(blk, acc[skip:, LANES:])
        else:
            top = wide if diag else 0
            cut = (top + blk) // 2
            put(0, acc[edge if diag else 0:, LANES:])
            lane = lax.broadcasted_iota(jnp.int32, (blk - cut, LANES), 1)
            put(LANES if diag else blk, jnp.where(lane < tail, pltpu.roll(acc[top:cut, :LANES], tail, 1), acc[cut:, :LANES]))

    def x_base(dest, slot, half):
        return pl.multiple_of((dest * slots + slot) * blk_rows + half * rows_l, 32)

    def ring_base(step, slot, way):
        off = (slot // 2) * blk_rows + (slot % 2) * (rows_l + way * (rows_s - rows_l))
        return pl.multiple_of((way * steps + step) * ring_rows + off, 32)

    def pair_copy(n, dest, slot, half, rows):
        return pltpu.make_async_remote_copy(
            src_ref=outgoing.at[pl.ds(pl.multiple_of((n % O_SLOTS) * rows_l, 32), rows)],
            dst_ref=x.at[pl.ds(x_base(dest, slot, half), rows)],
            send_sem=pair_send.at[n], recv_sem=pair_recv.at[n],
            device_id={"dp": partner}, device_id_type=MESH)

    def ring_copy(step, slot, way, dest, half, rows):
        target = up + way * (down - up)
        sem = (way * steps + step) * slots + slot
        return pltpu.make_async_remote_copy(
            src_ref=x.at[pl.ds(x_base(dest, slot, half), rows)],
            dst_ref=ring.at[pl.ds(ring_base(step, slot, way), rows)],
            send_sem=ring_send.at[sem], recv_sem=ring_recv.at[sem],
            device_id={"dp": target}, device_id_type=MESH)

    def wait_pair_send(n):
        _, slot, _, dest, half, valid = item(n)

        @pl.when(valid)
        def _():
            by_case(slot, half, lambda diag, part, rows: pair_copy(n, dest, slot, half, rows).wait_send())

    def for_partner(n):
        _, slot, _, dest, half, valid = item(n)

        @pl.when(n >= O_SLOTS)
        def _():
            wait_pair_send(n - O_SLOTS)

        @pl.when(valid)
        def _():
            multiply(dest, 1 - core, slot, half)
            base = (n % O_SLOTS) * rows_l

            def send(diag, part, rows):
                def put(row, value):
                    outgoing[pl.ds(pl.multiple_of(base + row, 32), value.shape[0]), :] = value

                emit(diag, part, put)
                pair_copy(n, dest, slot, half, rows).start()

            by_case(slot, half, send)

    def out_copy(slot):
        return pltpu.make_async_copy(stage.at[slot % 2], out_hbm.at[slot], out_sem.at[slot % 2])

    def finish(slot, diag, part, value):
        block = stage.at[slot % 2]
        if part == 0 and not diag:
            block[:, :LANES] = value(0, blk)
            block[:, LANES:wide] = value(blk, blk)
        elif part == 0:
            col0 = value(0, blk)
            col1 = value(blk, blk - LANES)
            block[:, :LANES] = col0
            block[LANES:, LANES:wide] = col1
            block[:LANES, LANES:wide] = col0[LANES:wide].T
            block[:LANES, wide:3 * LANES] = col0[wide:3 * LANES].T
            block[:LANES, 3 * LANES:] = col0[3 * LANES:].T
            block[LANES:wide, wide:3 * LANES] = col1[LANES:wide].T
            block[LANES:wide, 3 * LANES:] = col1[wide:].T
        else:
            top = wide if diag else 0
            cut = (blk - top) // 2
            tile = value(0, LANES if diag else blk)
            strip = value(LANES if diag else blk, cut)
            rolled = pltpu.roll(strip, tail, 1)
            if diag:
                across = jnp.concatenate([strip[tail:], rolled], axis=0)[:, :tail].T
                tile = jnp.concatenate([across, tile], axis=0)
            tile = pltpu.roll(tile, tail, 1)
            lane = lax.broadcasted_iota(jnp.int32, (cut, LANES), 1)
            block[top:top + cut, wide:3 * LANES] = jnp.where(lane < tail, strip, tile[:cut])
            block[top + cut:, wide:3 * LANES] = jnp.where(lane < tail, rolled, tile[cut:])
            block[top:, 3 * LANES:] = tile[:, :tail]

    def for_me(n):
        step, slot, way, dest, half, valid = item(n)

        @pl.when(valid)
        def _():
            multiply(dest, core, slot, half)
            base = x_base(dest, slot, half)

            def add(diag, part, rows):
                pair_copy(n, dest, slot, half, rows).wait_recv()

                def put(row, value):
                    span = pl.ds(pl.multiple_of(base + row, 32), value.shape[0])
                    x[span, :] = x[span, :] + value

                emit(diag, part, put)

                @pl.when(step > 0)
                def _():
                    ring_copy(step - 1, slot, way, dest, half, rows).wait_recv()

                r_base = ring_base(step - 1, slot, way)

                def value(row, size):
                    return (x[pl.ds(pl.multiple_of(base + row, 32), size), :]
                            + ring[pl.ds(pl.multiple_of(r_base + row, 32), size), :])

                @pl.when(jnp.logical_and(step > 0, step < steps))
                def _():
                    x[pl.ds(base, rows), :] = value(0, rows)

                @pl.when(step < steps)
                def _():
                    ring_copy(step, slot, way, dest, half, rows).start()

                @pl.when(step == steps)
                def _():
                    finish(slot, diag, part, value)

            @pl.when(jnp.logical_and(step == steps, jnp.logical_and(way == 0, slot >= 2)))
            def _():
                out_copy(slot - 2).wait()

            by_case(slot, half, add)

        @pl.when(jnp.logical_and(step == steps, jnp.logical_not(valid)))
        def _():
            @pl.when(way == 0)
            def _():
                out_copy(slot - 2).wait()
                stage[slot % 2] = jnp.zeros(stage.shape[1:], stage.dtype)

        @pl.when(jnp.logical_and(step == steps, way == 1))
        def _():
            out_copy(slot).start()

    load(first[0]).wait()
    for_partner(0)

    def body(n, carry):
        @pl.when(n == 0)
        def _():
            load(first[1]).wait()

        @pl.when(n == 1)
        def _():
            load(first[3]).wait()
            for index in rest:
                load(index).wait()

        @pl.when(n + 1 < n_items)
        def _():
            for_partner(n + 1)

        @pl.when(n == 0)
        def _():
            load(first[2]).wait()

        for_me(n)
        return carry

    lax.fori_loop(0, n_items, body, 0)

    def drain(n, carry):
        step, slot, way, dest, half, valid = item(n)

        @pl.when(valid)
        def _():
            by_case(slot, half, lambda diag, part, rows: ring_copy(step, slot, way, dest, half, rows).wait_send())

        return carry

    lax.fori_loop(0, steps * per_step, drain, 0)
    for n in range(n_items - O_SLOTS, n_items):
        wait_pair_send(n)
    for slot in (slots - 2, slots - 1):
        out_copy(slot).wait()


def solution(mesh):
    groups = mesh.shape["dp"]
    chips = groups // CORES
    slots = groups // 2 + 1

    def local_gram(a_local):
        n_rows, local_cols = a_local.shape
        blk = n_rows // groups
        rows_l, rows_s = 2 * blk, blk + blk // 2
        blk_rows = rows_l + rows_s
        ring_rows = groups // 4 * blk_rows + rows_l
        n_items = chips * 2 * slots
        n_ring = 2 * (chips - 1) * slots
        return pl.pallas_call(
            functools.partial(_kernel, groups, blk),
            out_shape=jax.ShapeDtypeStruct((slots, blk, blk), jnp.float32),
            in_specs=[pl.BlockSpec(memory_space=pl.ANY)],
            out_specs=pl.BlockSpec(memory_space=pl.ANY),
            scratch_shapes=[
                pltpu.VMEM((n_rows, local_cols), jnp.bfloat16),
                pltpu.VMEM((chips * slots * blk_rows, LANES), jnp.float32),
                pltpu.VMEM((2 * (chips - 1) * ring_rows, LANES), jnp.float32),
                pltpu.VMEM((O_SLOTS * rows_l, LANES), jnp.float32),
                pltpu.VMEM((blk, 2 * LANES), jnp.float32),
                pltpu.VMEM((2, blk, blk), jnp.float32),
                pltpu.SemaphoreType.DMA((groups,)),
                pltpu.SemaphoreType.DMA((n_items,)),
                pltpu.SemaphoreType.DMA((n_items,)),
                pltpu.SemaphoreType.DMA((n_ring,)),
                pltpu.SemaphoreType.DMA((n_ring,)),
                pltpu.SemaphoreType.DMA((2,)),
            ],
            compiler_params=pltpu.CompilerParams(
                collective_id=0, has_side_effects=True, vmem_limit_bytes=67_043_328),
        )(a_local)[None]

    return jax.shard_map(local_gram, mesh=mesh, in_specs=(P("mat", "dp"),), out_specs=P(("mat", "dp")), check_vma=False)
```

```python
import functools

import jax
import jax.numpy as jnp
from jax import lax
from jax.experimental import pallas as pl
from jax.experimental.pallas import tpu as pltpu
from jax.sharding import PartitionSpec as P

CORES = 2
LANES = 128
O_SLOTS = 4
VMEM_BYTES = 67_043_328
MESH = pl.DeviceIdType.MESH


def _diag_rows(blk):
    return 2 * blk - LANES, LANES + (blk - 2 * LANES) // 2


def _ring_rows(groups, blk):
    rows_dl, rows_ds = _diag_rows(blk)
    rows_l, rows_s = 2 * blk, blk + blk // 2
    middle = groups // 2 - 1
    return max(rows_dl + middle * rows_s + rows_l, rows_ds + middle * rows_l + rows_s)


def _store_kernel(src, out, hold, in_sem, out_sem):
    pieces = [(slot, pl.ds(part * hold.shape[1] // 2, hold.shape[1] // 2)) for slot in range(hold.shape[0]) for part in range(2)]
    loads = [pltpu.make_async_copy(src.at[slot, rows], hold.at[slot, rows], in_sem.at[n])
             for n, (slot, rows) in enumerate(pieces)]
    stores = [pltpu.make_async_copy(hold.at[slot, rows], out.at[slot, rows], out_sem.at[n])
              for n, (slot, rows) in enumerate(pieces)]
    for copy in loads:
        copy.start()
    for copy_in, copy_out in zip(loads, stores):
        copy_in.wait()
        copy_out.start()
    for copy in stores:
        copy.wait()


def _kernel(groups, blk, a_hbm, out_hbm, a, x, ring, outgoing, acc, stage,
            load_sem, pair_send, pair_recv, ring_send, ring_recv, out_sem):
    chips = groups // CORES
    half_groups = groups // 2
    slots = half_groups + 1
    steps = chips - 1
    per_step = 2 * slots
    n_items = chips * per_step
    wide = 2 * LANES
    mid = blk // 2
    rows_l, rows_s = 2 * blk, blk + mid
    edge = blk - LANES
    rows_dl, rows_ds = _diag_rows(blk)
    blk_rows = rows_l + rows_s
    ring_rows = _ring_rows(groups, blk)
    tail = edge - wide

    me = lax.axis_index("dp")
    chip, core = me // CORES, me % CORES
    partner = chip * CORES + 1 - core
    chip_up = (chip + 1) % chips
    chip_down = (chip + chips - 1) % chips
    up, down = chip_up * CORES + core, chip_down * CORES + core

    def row_block(index):
        return pl.ds(pl.multiple_of(index * blk, 64), blk)

    def load(index):
        return pltpu.make_async_copy(a_hbm.at[row_block(index)], a.at[row_block(index)], load_sem.at[index])

    chip_far = (chip + 2) % chips
    order = (chip_down * CORES + 1 - core, chip_up * CORES + 1 - core, chip_down * CORES + core, chip_up * CORES + core,
             chip_far * CORES + 1, chip * CORES + 1, chip_far * CORES, chip * CORES)
    for index in order[:2]:
        load(index).start()

    barrier = pltpu.get_barrier_semaphore()
    for other in (partner, up, down):
        pl.semaphore_signal(barrier, inc=1, device_id={"dp": other}, device_id_type=MESH)
    pl.semaphore_wait(barrier, 3)

    def item(n):
        step = n // per_step
        rest_n = n % per_step
        slot = rest_n // 2
        way = (rest_n + slot) % 2
        middle = (slot + groups - 1) // groups - slot // half_groups
        dest = (chip + 2 * chips + (1 + step) * (2 * way - 1)) % chips
        valid = jnp.logical_or(slot < half_groups, dest < chips // 2)
        return step, slot, way, dest, (middle + way) % 2, valid

    def by_case(slot, half, fn):
        for diag in (True, False):
            for part in (0, 1):
                cond = jnp.logical_and((slot == 0) if diag else (slot > 0), half == part)
                rows = ((rows_dl, rows_ds) if diag else (rows_l, rows_s))[part]
                pl.when(cond)(functools.partial(fn, diag, part, rows))

    def multiply(dest, parity, slot, half):
        p = dest * CORES + parity
        q = (p - slot + groups) % groups
        wrapped = (slot + groups - 1 - p) // groups
        hi = p + wrapped * (q - p)
        lo = q + wrapped * (p - q)
        right = pl.ds(pl.multiple_of(lo * blk + half * (blk - wide), 64), wide)
        corner = jnp.logical_and(slot == 0, half == 1)

        def product(top):
            left = pl.ds(pl.multiple_of(hi * blk + top, 64), blk - top)
            acc[top:, :] = lax.dot_general(a[left, :], a[right, :], (((1,), (1,)), ((), ())),
                                           preferred_element_type=jnp.float32)

        pl.when(corner)(functools.partial(product, wide))
        pl.when(jnp.logical_not(corner))(functools.partial(product, 0))

    def emit(diag, part, put):
        if part == 0:
            skip = LANES if diag else 0
            put(0, acc[:, :LANES])
            put(blk, acc[skip:, LANES:])
        else:
            top = wide if diag else 0
            cut = (top + blk) // 2
            put(0, acc[edge if diag else 0:, LANES:])
            lane = lax.broadcasted_iota(jnp.int32, (blk - cut, LANES), 1)
            put(LANES if diag else blk, jnp.where(lane < tail, pltpu.roll(acc[top:cut, :LANES], tail, 1), acc[cut:, :LANES]))

    def x_base(dest, slot, half):
        return pl.multiple_of((dest * slots + slot) * blk_rows + half * rows_l, 32)

    def ring_base(step, slot, way):
        first_rows = rows_dl + way * (rows_ds - rows_dl)
        other_rows = rows_s + way * (rows_l - rows_s)
        off = (slot + groups - 1) // groups * (first_rows + (slot - 1) * other_rows)
        return pl.multiple_of((way * steps + step) * ring_rows + off, 32)

    def pair_copy(n, dest, slot, half, rows):
        return pltpu.make_async_remote_copy(
            src_ref=outgoing.at[pl.ds(pl.multiple_of((n % O_SLOTS) * rows_l, 32), rows)],
            dst_ref=x.at[pl.ds(x_base(dest, slot, half), rows)],
            send_sem=pair_send.at[n], recv_sem=pair_recv.at[n],
            device_id={"dp": partner}, device_id_type=MESH)

    def ring_copy(step, slot, way, dest, half, rows):
        target = up + way * (down - up)
        sem = (way * steps + step) * slots + slot
        return pltpu.make_async_remote_copy(
            src_ref=x.at[pl.ds(x_base(dest, slot, half), rows)],
            dst_ref=ring.at[pl.ds(ring_base(step, slot, way), rows)],
            send_sem=ring_send.at[sem], recv_sem=ring_recv.at[sem],
            device_id={"dp": target}, device_id_type=MESH)

    def wait_pair_send(n):
        _, slot, _, dest, half, valid = item(n)

        @pl.when(valid)
        def _():
            by_case(slot, half, lambda diag, part, rows: pair_copy(n, dest, slot, half, rows).wait_send())

    def for_partner(n):
        _, slot, _, dest, half, valid = item(n)

        @pl.when(n >= O_SLOTS)
        def _():
            wait_pair_send(n - O_SLOTS)

        @pl.when(valid)
        def _():
            multiply(dest, 1 - core, slot, half)
            base = (n % O_SLOTS) * rows_l

            def send(diag, part, rows):
                def put(row, value):
                    outgoing[pl.ds(pl.multiple_of(base + row, 32), value.shape[0]), :] = value

                emit(diag, part, put)
                pair_copy(n, dest, slot, half, rows).start()

            by_case(slot, half, send)

    def out_copy(slot):
        return pltpu.make_async_copy(stage.at[slot % 2], out_hbm.at[slot], out_sem.at[slot % 2])

    def finish(slot, diag, part, value):
        block = stage.at[slot % 2]
        if part == 0 and not diag:
            block[:, :LANES] = value(0, blk)
            block[:, LANES:wide] = value(blk, blk)
        elif part == 0:
            col0 = value(0, blk)
            col1 = value(blk, blk - LANES)
            block[:, :LANES] = col0
            block[LANES:, LANES:wide] = col1
            block[:LANES, LANES:wide] = col0[LANES:wide].T
            block[:LANES, wide:3 * LANES] = col0[wide:3 * LANES].T
            block[:LANES, 3 * LANES:] = col0[3 * LANES:].T
            block[LANES:wide, wide:3 * LANES] = col1[LANES:wide].T
            block[LANES:wide, 3 * LANES:] = col1[wide:].T
        else:
            top = wide if diag else 0
            cut = (blk - top) // 2
            tile = value(0, LANES if diag else blk)
            strip = value(LANES if diag else blk, cut)
            rolled = pltpu.roll(strip, tail, 1)
            if diag:
                across = jnp.concatenate([strip[tail:], rolled], axis=0)[:, :tail].T
                tile = jnp.concatenate([across, tile], axis=0)
            tile = pltpu.roll(tile, tail, 1)
            lane = lax.broadcasted_iota(jnp.int32, (cut, LANES), 1)
            block[top:top + cut, wide:3 * LANES] = jnp.where(lane < tail, strip, tile[:cut])
            block[top + cut:, wide:3 * LANES] = jnp.where(lane < tail, rolled, tile[cut:])
            block[top:, 3 * LANES:] = tile[:, :tail]

    def for_me(n):
        step, slot, way, dest, half, valid = item(n)

        @pl.when(valid)
        def _():
            multiply(dest, core, slot, half)
            base = x_base(dest, slot, half)

            def add(diag, part, rows):
                pair_copy(n, dest, slot, half, rows).wait_recv()

                def put(row, value):
                    span = pl.ds(pl.multiple_of(base + row, 32), value.shape[0])
                    x[span, :] = x[span, :] + value

                emit(diag, part, put)

                @pl.when(step > 0)
                def _():
                    ring_copy(step - 1, slot, way, dest, half, rows).wait_recv()

                r_base = ring_base(step - 1, slot, way)

                def value(row, size):
                    return (x[pl.ds(pl.multiple_of(base + row, 32), size), :]
                            + ring[pl.ds(pl.multiple_of(r_base + row, 32), size), :])

                @pl.when(jnp.logical_and(step > 0, step < steps))
                def _():
                    x[pl.ds(base, rows), :] = value(0, rows)

                @pl.when(step < steps)
                def _():
                    ring_copy(step, slot, way, dest, half, rows).start()

                @pl.when(step == steps)
                def _():
                    finish(slot, diag, part, value)

            @pl.when(jnp.logical_and(step == steps, jnp.logical_and(n % 2 == 0, slot >= 2)))
            def _():
                out_copy(slot - 2).wait()

            by_case(slot, half, add)

        @pl.when(jnp.logical_and(step == steps, jnp.logical_not(valid)))
        def _():
            @pl.when(n % 2 == 0)
            def _():
                out_copy(slot - 2).wait()
                stage[slot % 2] = jnp.zeros(stage.shape[1:], stage.dtype)

        @pl.when(jnp.logical_and(step == steps, n % 2 == 1))
        def _():
            out_copy(slot).start()

    def ready(*places):
        for place in places:
            load(order[place]).wait()
            if place + 2 < groups:
                load(order[place + 2]).start()

    def body(n, carry):
        @pl.when(n == -1)
        def _():
            ready(0)

        @pl.when(n == 0)
        def _():
            ready(1)

        @pl.when(n == 1)
        def _():
            ready(3, 4, 5)

        @pl.when(n == 3)
        def _():
            ready(6, 7)

        @pl.when(n + 1 < n_items)
        def _():
            for_partner(n + 1)

        @pl.when(n == 0)
        def _():
            ready(2)

        @pl.when(n >= 0)
        def _():
            for_me(n)

        return carry

    lax.fori_loop(-1, n_items, body, 0)

    def drain(n, carry):
        step, slot, way, dest, half, valid = item(n)

        @pl.when(valid)
        def _():
            by_case(slot, half, lambda diag, part, rows: ring_copy(step, slot, way, dest, half, rows).wait_send())

        return carry

    lax.fori_loop(0, steps * per_step, drain, 0)
    for n in range(n_items - O_SLOTS, n_items):
        wait_pair_send(n)
    for slot in (slots - 2, slots - 1):
        out_copy(slot).wait()


def solution(mesh):
    groups = mesh.shape["dp"]
    chips = groups // CORES
    slots = groups // 2 + 1

    def local_gram(a_local):
        n_rows, local_cols = a_local.shape
        blk = n_rows // groups
        rows_l = 2 * blk
        blk_rows = 3 * blk + blk // 2
        ring_rows = _ring_rows(groups, blk)
        n_items = chips * 2 * slots
        n_ring = 2 * (chips - 1) * slots
        blocks = pl.pallas_call(
            functools.partial(_kernel, groups, blk),
            out_shape=jax.ShapeDtypeStruct((slots, blk, blk), jnp.float32),
            in_specs=[pl.BlockSpec(memory_space=pl.ANY)],
            out_specs=pl.BlockSpec(memory_space=pl.ANY),
            scratch_shapes=[
                pltpu.VMEM((n_rows, local_cols), jnp.bfloat16),
                pltpu.VMEM((chips * slots * blk_rows, LANES), jnp.float32),
                pltpu.VMEM((2 * (chips - 1) * ring_rows, LANES), jnp.float32),
                pltpu.VMEM((O_SLOTS * rows_l, LANES), jnp.float32),
                pltpu.VMEM((blk, 2 * LANES), jnp.float32),
                pltpu.VMEM((2, blk, blk), jnp.float32),
                pltpu.SemaphoreType.DMA((groups,)),
                pltpu.SemaphoreType.DMA((n_items,)),
                pltpu.SemaphoreType.DMA((n_items,)),
                pltpu.SemaphoreType.DMA((n_ring,)),
                pltpu.SemaphoreType.DMA((n_ring,)),
                pltpu.SemaphoreType.DMA((2,)),
            ],
            compiler_params=pltpu.CompilerParams(
                collective_id=0, has_side_effects=True, vmem_limit_bytes=VMEM_BYTES),
        )(a_local)
        stored = pl.pallas_call(
            _store_kernel,
            out_shape=jax.ShapeDtypeStruct(blocks.shape, blocks.dtype),
            in_specs=[pl.BlockSpec(memory_space=pl.ANY)],
            out_specs=pl.BlockSpec(memory_space=pl.ANY),
            scratch_shapes=[
                pltpu.VMEM(blocks.shape, blocks.dtype),
                pltpu.SemaphoreType.DMA((2 * slots,)),
                pltpu.SemaphoreType.DMA((2 * slots,)),
            ],
            compiler_params=pltpu.CompilerParams(vmem_limit_bytes=VMEM_BYTES),
        )(blocks)
        return stored[None]

    return jax.shard_map(local_gram, mesh=mesh, in_specs=(P("mat", "dp"),), out_specs=P(("mat", "dp")), check_vma=False)
```

```python
import functools

import jax
import jax.numpy as jnp
from jax import lax
from jax.experimental import pallas as pl
from jax.experimental.pallas import tpu as pltpu
from jax.sharding import PartitionSpec as P

CORES = 2
LANES = 128
O_SLOTS = 4
VMEM_BYTES = 67_043_328
MESH = pl.DeviceIdType.MESH


class _Pieces:
    HEAD, SIDE, CORNER, LEFT, RIGHT = range(5)

    def __init__(self, groups, blk):
        wide = 2 * LANES
        low = blk - wide
        self.rows = (wide + LANES, 2 * low, LANES + low // 2, 2 * blk, blk + blk // 2)
        self.block = self.rows[self.LEFT] + self.rows[self.RIGHT]
        self.at = (0, self.rows[self.HEAD], self.rows[self.LEFT], 0, self.rows[self.LEFT])
        half = groups // 2
        self.slots = half + 1
        middle = half - 1
        self.ways = (
            [self.HEAD, self.SIDE] + [self.RIGHT] * middle + [self.LEFT],
            [self.CORNER] + [self.LEFT] * middle + [self.RIGHT],
        )
        self.places = len(self.ways[0])
        self.ring = max(sum(self.rows[kind] for kind in way) for way in self.ways)


def _store_kernel(src, out, hold, in_sem, out_sem):
    pieces = [(slot, pl.ds(part * hold.shape[1] // 2, hold.shape[1] // 2)) for slot in range(hold.shape[0]) for part in range(2)]
    loads = [pltpu.make_async_copy(src.at[slot, rows], hold.at[slot, rows], in_sem.at[n])
             for n, (slot, rows) in enumerate(pieces)]
    stores = [pltpu.make_async_copy(hold.at[slot, rows], out.at[slot, rows], out_sem.at[n])
              for n, (slot, rows) in enumerate(pieces)]
    for copy in loads:
        copy.start()
    for copy_in, copy_out in zip(loads, stores):
        copy_in.wait()
        copy_out.start()
    for copy in stores:
        copy.wait()


def _kernel(groups, blk, a_hbm, out_hbm, a, x, ring, outgoing, acc, stage,
            load_sem, pair_send, pair_recv, ring_send, ring_recv, out_sem):
    pieces = _Pieces(groups, blk)
    HEAD, SIDE, CORNER, LEFT, RIGHT = range(5)
    chips = groups // CORES
    half_groups = groups // 2
    slots, places = pieces.slots, pieces.places
    steps = chips - 1
    per_step = 2 * places
    n_items = chips * per_step
    wide = 2 * LANES
    edge = blk - LANES
    tail = edge - wide
    low = blk - wide
    mid = blk // 2
    rows_l = pieces.rows[LEFT]

    me = lax.axis_index("dp")
    chip, core = me // CORES, me % CORES
    partner = chip * CORES + 1 - core
    chip_up = (chip + 1) % chips
    chip_down = (chip + chips - 1) % chips
    chip_far = (chip + 2) % chips
    up, down = chip_up * CORES + core, chip_down * CORES + core

    cuts = (0, wide - tail, wide, blk)

    def load(index, parts):
        begin, end = cuts[parts[0]], cuts[parts[-1] + 1]
        rows = pl.ds(pl.multiple_of(index * blk + begin, 64), end - begin)
        return pltpu.make_async_copy(a_hbm.at[rows], a.at[rows], load_sem.at[index, parts[0]])

    whole, top, strip, bottom = (0, 1, 2), (0,), (1,), (2,)
    down_other, down_same = chip_down * CORES + 1 - core, chip_down * CORES + core
    up_other, up_same = chip_up * CORES + 1 - core, chip_up * CORES + core
    loads = (
        [load(down_other, top), load(down_other, strip)],
        [load(up_other, strip), load(up_other, bottom)],
        [load(down_same, top), load(down_same, strip)],
        [load(up_same, strip), load(up_same, bottom)],
        [load(up_other, top), load(up_same, top), load(chip * CORES + 1, whole)],
        [load(down_other, bottom)],
        [load(down_same, bottom)],
        [load(chip_far * CORES + 1, whole)],
        [load(chip * CORES, whole)],
        [load(chip_far * CORES, whole)],
    )
    for batch in loads:
        for copy in batch:
            copy.start()

    def ready(n, batches):
        for at, batch in batches.items():
            @pl.when(n == at)
            def _(batch=batch):
                for copy in loads[batch]:
                    copy.wait()

    ready_partner = functools.partial(ready, batches={0: 0, 1: 1, 2: 4, 3: 5, 4: 7, 5: 8, 6: 9})
    ready_mine = functools.partial(ready, batches={0: 2, 1: 3, 3: 6})

    barrier = pltpu.get_barrier_semaphore()
    for other in (partner, up, down):
        pl.semaphore_signal(barrier, inc=1, device_id={"dp": other}, device_id_type=MESH)
    pl.semaphore_wait(barrier, 3)

    def item(n):
        step = n // per_step
        place = n % per_step // 2
        way = (n + place) % 2
        dest = (chip + 2 * chips + (1 + step) * (2 * way - 1)) % chips
        after = (place + places - 1) // places
        slot = place - (1 - way) * after
        in_table = jnp.logical_or(way == 0, place < places - 1)
        valid = jnp.logical_and(in_table, jnp.logical_or(slot < half_groups, dest < chips // 2))
        return step, place, way, dest, slot, valid

    def by_case(place, way, fn):
        cases = {}
        for table_way, kinds in enumerate(pieces.ways):
            for at, kind in enumerate(kinds):
                cases.setdefault(kind, []).append((table_way, at))
        for kind, spots in cases.items():
            cond = False
            for table_way in (0, 1):
                ats = [at for w, at in spots if w == table_way]
                if ats:
                    hit = jnp.logical_and(way == table_way, jnp.logical_and(place >= min(ats), place <= max(ats)))
                    cond = hit if cond is False else jnp.logical_or(cond, hit)
            pl.when(cond)(functools.partial(fn, kind))

    def multiply(dest, parity, slot, place, way):
        p = dest * CORES + parity
        q = (p - slot + groups) % groups
        wrapped = (slot + groups - 1 - p) // groups
        hi = p + wrapped * (q - p)
        lo = q + wrapped * (p - q)

        def product(begin, end, shift):
            left = pl.ds(pl.multiple_of(hi * blk + begin, 64), end - begin)
            right = pl.ds(pl.multiple_of(lo * blk + shift, 64), wide)
            acc[begin:end, :] = lax.dot_general(a[left, :], a[right, :], (((1,), (1,)), ((), ())),
                                                preferred_element_type=jnp.float32)

        head = jnp.logical_and(slot == 0, jnp.logical_and(way == 0, place == 0))
        below = jnp.logical_and(slot == 0, jnp.logical_not(head))
        last = (place + 1) // places
        right_half = jnp.where(way == 0, 1 - last, place // (places - 2))
        pl.when(head)(functools.partial(product, 0, wide, 0))
        pl.when(below)(functools.partial(product, wide, blk, way * low))
        pl.when(slot > 0)(functools.partial(product, 0, blk, right_half * low))

    lane_of = lambda n: lax.broadcasted_iota(jnp.int32, (n, LANES), 1)

    def emit(kind, put):
        if kind in (HEAD, SIDE, LEFT):
            begin, end = {HEAD: (0, wide), SIDE: (wide, blk), LEFT: (0, blk)}[kind]
            put(0, acc[begin:end, :LANES])
            put(end - begin, acc[LANES if kind == HEAD else begin:end, LANES:])
        else:
            begin = wide if kind == CORNER else 0
            cut = (begin + blk) // 2
            full = edge if kind == CORNER else 0
            put(0, acc[full:, LANES:])
            put(blk - full, jnp.where(lane_of(blk - cut) < tail, pltpu.roll(acc[begin:cut, :LANES], tail, 1), acc[cut:, :LANES]))

    def spot(kind, place):
        kinds = pieces.ways[0 if kind in (HEAD, SIDE) else 1]
        if kind in (HEAD, SIDE, CORNER):
            return sum(pieces.rows[k] for k in kinds[:kinds.index(kind)])
        return None

    def x_base(kind, dest, slot):
        return pl.multiple_of((dest * slots + slot) * pieces.block + pieces.at[kind], 32)

    def ring_base(kind, step, place, way):
        if spot(kind, place) is not None:
            off = spot(kind, place)
        else:
            size = pieces.rows
            up_off = size[HEAD] + size[SIDE] + (place - 2) * size[RIGHT]
            down_off = size[CORNER] + (place - 1) * size[LEFT]
            off = up_off + way * (down_off - up_off)
        return pl.multiple_of((way * steps + step) * pieces.ring + off, 32)

    def pair_copy(kind, n, dest, slot):
        rows = pieces.rows[kind]
        return pltpu.make_async_remote_copy(
            src_ref=outgoing.at[pl.ds(pl.multiple_of((n % O_SLOTS) * rows_l, 32), rows)],
            dst_ref=x.at[pl.ds(x_base(kind, dest, slot), rows)],
            send_sem=pair_send.at[n], recv_sem=pair_recv.at[n],
            device_id={"dp": partner}, device_id_type=MESH)

    def ring_copy(kind, step, place, way, dest, slot):
        rows = pieces.rows[kind]
        target = up + way * (down - up)
        sem = (way * steps + step) * places + place
        return pltpu.make_async_remote_copy(
            src_ref=x.at[pl.ds(x_base(kind, dest, slot), rows)],
            dst_ref=ring.at[pl.ds(ring_base(kind, step, place, way), rows)],
            send_sem=ring_send.at[sem], recv_sem=ring_recv.at[sem],
            device_id={"dp": target}, device_id_type=MESH)

    def wait_pair_send(n):
        _, place, way, dest, slot, valid = item(n)

        @pl.when(valid)
        def _():
            by_case(place, way, lambda kind: pair_copy(kind, n, dest, slot).wait_send())

    def for_partner(n):
        _, place, way, dest, slot, valid = item(n)

        @pl.when(n >= O_SLOTS)
        def _():
            wait_pair_send(n - O_SLOTS)

        @pl.when(valid)
        def _():
            multiply(dest, 1 - core, slot, place, way)
            base = (n % O_SLOTS) * rows_l

            def send(kind):
                def put(row, value):
                    outgoing[pl.ds(pl.multiple_of(base + row, 32), value.shape[0]), :] = value

                emit(kind, put)
                pair_copy(kind, n, dest, slot).start()

            by_case(place, way, send)

    def out_copy(slot):
        return pltpu.make_async_copy(stage.at[slot % 2], out_hbm.at[slot], out_sem.at[slot % 2])

    def finish(kind, slot, value):
        block = stage.at[slot % 2]
        if kind == LEFT:
            block[:, :LANES] = value(0, blk)
            block[:, LANES:wide] = value(blk, blk)
        elif kind == HEAD:
            col0 = value(0, wide)
            block[:wide, :LANES] = col0
            block[LANES:wide, LANES:wide] = value(wide, LANES)
            block[:LANES, LANES:wide] = col0[LANES:].T
        elif kind == SIDE:
            for part in (0, 1):
                col = value(part * low, low)
                lanes = slice(part * LANES, (part + 1) * LANES)
                block[wide:, lanes] = col
                block[lanes, wide:wide + LANES] = col[:LANES].T
                block[lanes, wide + LANES:] = col[LANES:].T
        else:
            begin = wide if kind == CORNER else 0
            full = LANES if kind == CORNER else blk
            cut = (blk - begin) // 2
            tile = value(0, full)
            packed = value(full, cut)
            rolled = pltpu.roll(packed, tail, 1)
            if kind == CORNER:
                across = jnp.concatenate([packed[tail:], rolled], axis=0)[:, :tail].T
                tile = jnp.concatenate([across, tile], axis=0)
            tile = pltpu.roll(tile, tail, 1)
            lane = lane_of(cut)
            block[begin:begin + cut, wide:3 * LANES] = jnp.where(lane < tail, packed, tile[:cut])
            block[begin + cut:, wide:3 * LANES] = jnp.where(lane < tail, rolled, tile[cut:])
            block[begin:, 3 * LANES:] = tile[:, :tail]

    def for_me(n):
        step, place, way, dest, slot, valid = item(n)
        final = step == steps

        @pl.when(jnp.logical_and(final, jnp.logical_and(way == 1, jnp.logical_and(place >= 2, place < slots))))
        def _():
            out_copy(place - 2).wait()

        @pl.when(valid)
        def _():
            multiply(dest, core, slot, place, way)

            def add(kind):
                rows = pieces.rows[kind]
                base = x_base(kind, dest, slot)
                pair_copy(kind, n, dest, slot).wait_recv()

                def put(row, value):
                    span = pl.ds(pl.multiple_of(base + row, 32), value.shape[0])
                    x[span, :] = x[span, :] + value

                emit(kind, put)

                @pl.when(step > 0)
                def _():
                    ring_copy(kind, step - 1, place, way, dest, slot).wait_recv()

                r_base = ring_base(kind, step - 1, place, way)

                def value(row, size):
                    return (x[pl.ds(pl.multiple_of(base + row, 32), size), :]
                            + ring[pl.ds(pl.multiple_of(r_base + row, 32), size), :])

                @pl.when(jnp.logical_and(step > 0, step < steps))
                def _():
                    x[pl.ds(base, rows), :] = value(0, rows)

                @pl.when(step < steps)
                def _():
                    ring_copy(kind, step, place, way, dest, slot).start()

                @pl.when(final)
                def _():
                    finish(kind, slot, value)

            by_case(place, way, add)

        @pl.when(jnp.logical_and(final, jnp.logical_and(way == 0, place >= 1)))
        def _():
            @pl.when(jnp.logical_not(valid))
            def _():
                stage[slot % 2] = jnp.zeros(stage.shape[1:], stage.dtype)

            out_copy(slot).start()

    def pair(index, carry):
        def partner_item(turn, inner):
            ready_partner(2 * index + turn)
            for_partner(2 * index + turn)
            return inner

        def my_item(turn, inner):
            ready_mine(2 * index + turn)
            for_me(2 * index + turn)
            return inner

        lax.fori_loop(0, 2, partner_item, 0)
        lax.fori_loop(0, 2, my_item, 0)
        return carry

    lax.fori_loop(0, n_items // 2, pair, 0)

    def drain(n, carry):
        step, place, way, dest, slot, valid = item(n)

        @pl.when(valid)
        def _():
            by_case(place, way, lambda kind: ring_copy(kind, step, place, way, dest, slot).wait_send())

        return carry

    lax.fori_loop(0, steps * per_step, drain, 0)
    for n in range(n_items - O_SLOTS, n_items):
        wait_pair_send(n)
    for slot in (slots - 2, slots - 1):
        out_copy(slot).wait()


def solution(mesh):
    groups = mesh.shape["dp"]
    chips = groups // CORES

    def local_gram(a_local):
        n_rows, local_cols = a_local.shape
        blk = n_rows // groups
        pieces = _Pieces(groups, blk)
        slots = pieces.slots
        n_items = chips * 2 * pieces.places
        n_ring = 2 * (chips - 1) * pieces.places
        blocks = pl.pallas_call(
            functools.partial(_kernel, groups, blk),
            out_shape=jax.ShapeDtypeStruct((slots, blk, blk), jnp.float32),
            in_specs=[pl.BlockSpec(memory_space=pl.ANY)],
            out_specs=pl.BlockSpec(memory_space=pl.ANY),
            scratch_shapes=[
                pltpu.VMEM((n_rows, local_cols), jnp.bfloat16),
                pltpu.VMEM((chips * slots * pieces.block, LANES), jnp.float32),
                pltpu.VMEM((2 * (chips - 1) * pieces.ring, LANES), jnp.float32),
                pltpu.VMEM((O_SLOTS * pieces.rows[pieces.LEFT], LANES), jnp.float32),
                pltpu.VMEM((blk, 2 * LANES), jnp.float32),
                pltpu.VMEM((2, blk, blk), jnp.float32),
                pltpu.SemaphoreType.DMA((groups, 3)),
                pltpu.SemaphoreType.DMA((n_items,)),
                pltpu.SemaphoreType.DMA((n_items,)),
                pltpu.SemaphoreType.DMA((n_ring,)),
                pltpu.SemaphoreType.DMA((n_ring,)),
                pltpu.SemaphoreType.DMA((2,)),
            ],
            compiler_params=pltpu.CompilerParams(
                collective_id=0, has_side_effects=True, vmem_limit_bytes=VMEM_BYTES),
        )(a_local)
        stored = pl.pallas_call(
            _store_kernel,
            out_shape=jax.ShapeDtypeStruct(blocks.shape, blocks.dtype),
            in_specs=[pl.BlockSpec(memory_space=pl.ANY)],
            out_specs=pl.BlockSpec(memory_space=pl.ANY),
            scratch_shapes=[
                pltpu.VMEM(blocks.shape, blocks.dtype),
                pltpu.SemaphoreType.DMA((2 * slots,)),
                pltpu.SemaphoreType.DMA((2 * slots,)),
            ],
            compiler_params=pltpu.CompilerParams(vmem_limit_bytes=VMEM_BYTES),
        )(blocks)
        return stored[None]

    return jax.shard_map(local_gram, mesh=mesh, in_specs=(P("mat", "dp"),), out_specs=P(("mat", "dp")), check_vma=False)
```
